32 devices in a mesh: dp: 4 (over x, core), tensor: 8 (over z, y).
Axes of the slice: x: 2, y: 2, z: 4, core: 2. Of those that a mesh axis runs over, the one named last changes fastest.
Arguments:
- hidden: bfloat16 [8, 64, 4608], P('dp', 'tensor'), may hold values from -6 to 6
- gain: float32 [4608], replicated, may hold values from 0.5 to 1.5
- labels: int32 [8, 64], P('dp', 'tensor'), may hold values from 0 to 255999
- lengths: int32 [8], replicated, may hold values from 1 to 64
- embed: bfloat16 [256000, 4608], P(('dp', 'tensor')), may hold values from -0.375 to 0.375
Outputs:
- token_logprob: float32 [8, 64], P('dp', 'tensor')
- mean_nll: float32 [], replicated
- z_loss: float32 [], replicated
The draws below stay inside these ranges and needn't reach their ends.
All inputs are finite; a program needn't handle non-finite values.
Results may differ from the reference program's by a relative error of at most 0.00058.
Values may be sent and summed in bfloat16 or wider, within the bound.
A program may use at most 128 MiB of HBM per device.

```python
import jax
import jax.numpy as jnp
from jax import lax

D = 4608
VOCAB = 256000
CAP = 30
LENGTH = 64
BATCH = 8


def set_ends(drawn, stream_key, least, largest):
    longest = drawn.shape.index(max(drawn.shape))
    spots = []
    for shift in (0, 1):
        where = [jax.random.randint(jax.random.fold_in(stream_key, axis), (), 0, length) for axis, length in enumerate(drawn.shape)]
        where[longest] = (where[longest] + shift) % drawn.shape[longest]
        spots.append(tuple(where))
    return drawn.at[spots[0]].set(least).at[spots[1]].set(largest)


def steps_of(key, dims, split, low, high):
    loudness = 1.0
    for axis_at, shards_of in split:
        steps = jax.random.uniform(jax.random.fold_in(jax.random.fold_in(key, 6), axis_at), (shards_of,), jnp.float32, low / len(split), high / len(split))
        loudness = loudness * jnp.repeat(jnp.exp(steps), dims[axis_at] // shards_of).reshape((-1,) + (1,) * (len(dims) - 1 - axis_at))
    return loudness


def normal_values(rng, dims, deviation, reach, pieces=(), dtype=jnp.bfloat16):
    drawn = jax.random.normal(rng, dims, jnp.float32) * deviation
    if len(pieces) > 0:
        drawn = steps_of(rng, dims, pieces, -0.22, 0.18) * drawn
    return jnp.clip(drawn, min=-reach, max=reach).astype(dtype)


def setup_inputs(seed: int = 0) -> dict:
    splits = jax.random.split(jax.random.key(seed), 6)
    hidden = normal_values(splits[0], (BATCH, LENGTH, D), 1.0, 6.0, ((0, 4), (1, 8)))
    gain = jnp.clip(1.0 + 0.1 * jax.random.normal(splits[1], (D,), jnp.float32), 0.5, 1.5)
    labels = set_ends(jax.random.randint(splits[2], (BATCH, LENGTH), 0, VOCAB), jax.random.fold_in(splits[2], 1), 0, VOCAB - 1).astype(jnp.int32)
    lengths = set_ends(jax.random.randint(splits[3], (BATCH,), 1, LENGTH + 1), jax.random.fold_in(splits[3], 1), 1, LENGTH).astype(jnp.int32)
    embed = normal_values(splits[4], (VOCAB, D), (D // 16) ** -0.5, 0.375, ((0, 32),))
    return dict(hidden=hidden, gain=gain, labels=labels, lengths=lengths, embed=embed)


def normalize(rows, gain):
    values = rows.astype(jnp.float32)
    meansq = lax.optimization_barrier(jnp.mean(values * values, axis=-1, keepdims=True))
    return (values * lax.rsqrt(meansq + 1e-06) * gain).astype(jnp.bfloat16)

def reference(hidden, gain, labels, lengths, embed):
    total_rows = BATCH * LENGTH
    normed = normalize(hidden.reshape(total_rows, D), gain)
    flat_labels = labels.reshape(total_rows)
    blocks = 32
    width = VOCAB // blocks
    table = embed.reshape(blocks, width, D)

    def visit(carry, item):
        sumexp, picked = carry
        tile, offset = item
        raw = lax.dot_general(normed, tile, (((1,), (1,)), ((), ())), preferred_element_type=jnp.float32)
        capped = CAP * jnp.tanh(raw / CAP)
        sumexp = sumexp + lax.optimization_barrier(jnp.sum(jnp.exp(capped), axis=1))
        local = flat_labels - offset
        inside = (local >= 0) & (local < width)
        chosen = jnp.take_along_axis(capped, jnp.clip(local, 0, width - 1)[:, None], axis=1)[:, 0]
        picked = picked + jnp.where(inside, chosen, jnp.float32(0.0))
        return ((sumexp, picked), None)
    offsets = (jnp.arange(blocks) * width).astype(jnp.int32)
    start = (jnp.zeros((total_rows,), jnp.float32), jnp.zeros((total_rows,), jnp.float32))
    (sumexp, picked), _ = lax.scan(visit, start, (table, offsets))
    lse = jnp.log(sumexp)
    positions = jnp.arange(LENGTH).astype(jnp.int32)
    live = (positions[None, :] < lengths[:, None]).astype(jnp.float32).reshape(total_rows)
    token = live * (picked - lse)
    count = jnp.sum(live)
    mean_nll = -jnp.sum(token) / count
    z_loss = 0.01 * jnp.sum(live * lse * lse) / count
    return (token.reshape(BATCH, LENGTH), mean_nll, z_loss)
```

```python
import functools
import math

import jax
import jax.numpy as jnp
from jax import lax
from jax.experimental import pallas as pl
from jax.experimental.pallas import tpu as pltpu
from jax.sharding import PartitionSpec as P

CAP = 30
LANES = 128
CHUNK = 256
MESH = pl.DeviceIdType.MESH


def tile_rows(vocab_dev):
    best = 16
    for size in range(16, 513, 16):
        if vocab_dev % size == 0:
            best = size
    return best


def kernel(
    cfg, hidden_ref, gain_ref, labels_ref, lengths_ref, embed_ref, out_ref,
    rows, tiles, acc0, acc1, sums, picks, labs, labrow, labels_all, mine, parts,
    tile_sem, ring_send, ring_recv, mate_send, mate_recv, lab_send, lab_recv, fin_send, fin_recv,
):
    n_dp, n_t, half, seqs, stretch, vt, n_tiles, n_slots, last, early = cfg
    n_all = n_dp * n_t
    chips = n_all // 2
    passes = chips * 2 * half // CHUNK
    per_pass = CHUNK // half
    dp, tt = lax.axis_index("dp"), lax.axis_index("tensor")
    me = dp * n_t + tt
    core = lax.rem(dp, 2)

    def swap(i):
        return i + lax.rem(i // 2, 2) * (1 - 2 * lax.rem(i, 2))

    def ring_of(x, t):
        q = swap(t)
        odd = lax.rem(x, 2)
        return x * n_t + q + odd * (n_t - 1 - 2 * q)

    def chip_of(r):
        x = r // n_t
        q = lax.rem(r, n_t)
        odd = lax.rem(x, 2)
        return x, swap(q + odd * (n_t - 1 - 2 * q))

    here = ring_of(dp // 2, tt)
    next_x, next_t = chip_of(lax.rem(here + 1 - 2 * core + chips, chips))
    next_dev = {"dp": next_x * 2 + core, "tensor": next_t}
    mate_dev = {"dp": dp + 1 - 2 * core, "tensor": tt}
    reach = last - core
    mate_reach = last - 1 + core

    def slot_of(d, side):
        return jnp.where(d == 0, 0, 2 * d - 1 + side)

    def block(slot, h):
        return rows.at[pl.ds(pl.multiple_of((slot * 2 + h) * half, half), half), :]

    def to_next(d, h):
        return pltpu.make_async_remote_copy(
            src_ref=block(slot_of(d, core), h), dst_ref=block(slot_of(d + 1, core), h),
            send_sem=ring_send.at[d, h], recv_sem=ring_recv.at[d + 1, h],
            device_id=next_dev, device_id_type=MESH)

    def from_last(d, h):
        return pltpu.make_async_remote_copy(
            src_ref=block(slot_of(d, core), h), dst_ref=block(slot_of(d, core), h),
            send_sem=ring_send.at[d, h], recv_sem=ring_recv.at[d, h],
            device_id=next_dev, device_id_type=MESH)

    def to_mate(d, h):
        return pltpu.make_async_remote_copy(
            src_ref=block(slot_of(d, core), h), dst_ref=block(slot_of(d, core), h),
            send_sem=mate_send.at[d, h], recv_sem=mate_recv.at[d, h],
            device_id=mate_dev, device_id_type=MESH)

    def from_mate(d, h):
        return pltpu.make_async_remote_copy(
            src_ref=block(slot_of(d, 1 - core), h), dst_ref=block(slot_of(d, 1 - core), h),
            send_sem=mate_send.at[d, h], recv_sem=mate_recv.at[d, h],
            device_id=mate_dev, device_id_type=MESH)

    def fetch(t):
        slot = lax.rem(t, n_slots)
        return pltpu.make_async_copy(
            embed_ref.at[pl.ds(pl.multiple_of(t * vt, vt), vt), :], tiles.at[slot], tile_sem.at[slot])

    def label_copy(source, target):
        return pltpu.make_async_remote_copy(
            src_ref=labels_ref, dst_ref=labels_all.at[source],
            send_sem=lab_send.at[target], recv_sem=lab_recv.at[source],
            device_id={"dp": target // n_t, "tensor": lax.rem(target, n_t)}, device_id_type=MESH)

    def part_copy(source, target):
        return pltpu.make_async_remote_copy(
            src_ref=mine, dst_ref=parts.at[source],
            send_sem=fin_send.at[target], recv_sem=fin_recv.at[source],
            device_id={"dp": target // n_t, "tensor": lax.rem(target, n_t)}, device_id_type=MESH)

    def others(visit):
        def body(k, carry):
            visit(lax.rem(me + k, n_all))
            return carry
        lax.fori_loop(1, n_all, body, 0)

    values = hidden_ref[...].astype(jnp.float32)
    meansq = jnp.mean(values * values, axis=-1, keepdims=True)
    rows[pl.ds(pl.multiple_of(core * half, half), half), :] = (
        values * lax.rsqrt(meansq + 1e-06) * gain_ref[...]).astype(jnp.bfloat16)

    barrier = pltpu.get_barrier_semaphore()
    others(lambda j: pl.semaphore_signal(
        barrier, inc=1, device_id={"dp": j // n_t, "tensor": lax.rem(j, n_t)}, device_id_type=MESH))

    def first_fetch(t, carry):
        fetch(t).start()
        return carry
    lax.fori_loop(0, n_slots, first_fetch, 0)

    sums[...] = jnp.zeros_like(sums)
    picks[...] = jnp.zeros_like(picks)
    acc1[...] = jnp.zeros_like(acc1)
    labels_all[me] = labels_ref[...]
    pl.semaphore_wait(barrier, n_all - 1)

    to_next(0, core).start()
    to_mate(0, core).start()
    others(lambda j: label_copy(me, j).start())
    from_mate(0, 1 - core).wait_recv()
    to_next(0, 1 - core).start()

    def ring_step(step):
        d = step // 2 + 1
        h = lax.rem(core + lax.rem(step, 2), 2)

        @pl.when(d <= reach)
        def _():
            from_last(d, h).wait_recv()
            to_mate(d, h).start()

            @pl.when(d < reach)
            def _():
                to_next(d, h).start()

    def ring_body(step, carry):
        ring_step(step)
        return carry

    def mate_body(step, carry):
        d = step // 2 + 1

        @pl.when(d <= mate_reach)
        def _():
            from_mate(d, lax.rem(core + 1 + lax.rem(step, 2), 2)).wait_recv()
        return carry

    lax.fori_loop(0, 2 * early, ring_body, 0)

    others(lambda j: label_copy(j, me).wait_recv())
    lane = lax.broadcasted_iota(jnp.int32, (1, LANES), 1)
    group = LANES // half

    def device_at(index):
        slot = index // 2
        d = (slot + 1) // 2
        away = jnp.where(lax.rem(slot, 2) == 1, chips - d, d)
        x, t = chip_of(lax.rem(here + away, chips))
        return (x * 2 + lax.rem(index, 2)) * n_t + t

    def place_labels(row, carry):
        total = jnp.zeros((1, LANES), jnp.int32)
        for b in range(group):
            total = jnp.where(lane // half == b, labels_all[device_at(row * group + b)], total)
        labrow[row] = total
        return carry
    lax.fori_loop(0, passes * CHUNK // LANES, place_labels, 0)
    for p in range(passes):
        labs[p] = jnp.concatenate([labrow[p * (CHUNK // LANES) + i] for i in range(CHUNK // LANES)], axis=1)

    lax.fori_loop(0, 2 * early, mate_body, 0)

    first = me * (vt * n_tiles)
    late = 2 * (last - early)

    def where_of(v):
        p = v // n_tiles
        q = lax.rem(v, n_tiles)
        odd = lax.rem(p, 2)
        return p, q, jnp.where(odd == 1, n_tiles - 1 - q, q)

    def score(acc, p, slot, t):
        th = jnp.tanh(acc[...] * (1.0 / CAP))
        grown = jnp.exp2(th * (CAP * math.log2(math.e)))
        local = labs[p] - (first + t * vt)
        chosen = jnp.where(lax.broadcasted_iota(jnp.int32, (vt, CHUNK), 0) == local, th, 0.0)
        sums[slot] += jnp.sum(grown.reshape(vt // 8, 8, CHUNK), axis=0)
        picks[slot] += jnp.sum(chosen.reshape(vt // 8, 8, CHUNK), axis=0)

    def visit(v, acc, before):
        p, q, t = where_of(v)
        slot = lax.rem(t, n_slots)

        @pl.when((v < n_tiles) | (q >= n_slots))
        def _():
            fetch(t).wait()

        if late > 0:
            @pl.when((v < n_tiles) & (lax.rem(v, 2) == 1) & (v // 2 < late))
            def _():
                ring_step(2 * early + v // 2)

            @pl.when(v == n_tiles)
            def _():
                lax.fori_loop(2 * early, 2 * last, mate_body, 0)

        @pl.when((v > 0) & (lax.rem(v - 1, n_tiles) + n_slots < n_tiles))
        def _():
            _, _, used = where_of(v - 1)
            odd = lax.rem((v - 1) // n_tiles, 2)
            fetch(used + n_slots - 2 * odd * n_slots).start()

        product = lax.dot_general(
            tiles[slot], rows[pl.ds(pl.multiple_of(p * CHUNK, CHUNK), CHUNK), :],
            (((1,), (1,)), ((), ())), preferred_element_type=jnp.float32)
        vb = jnp.maximum(v - 1, 0)
        pb, _, tb = where_of(vb)
        score(before, pb, jnp.where(v == 0, passes, pb), tb)
        acc[...] = product

    def pair(i, carry):
        visit(2 * i, acc0, acc1)
        visit(2 * i + 1, acc1, acc0)
        return carry
    lax.fori_loop(0, passes * n_tiles // 2, pair, 0)
    end = passes * n_tiles - 1
    p_end, _, t_end = where_of(jnp.int32(end))
    score(acc1, p_end, p_end, t_end)

    n_rows = passes * CHUNK // LANES
    for p in range(passes):
        total = jnp.sum(sums[p], axis=0, keepdims=True)
        chosen = jnp.sum(picks[p], axis=0, keepdims=True)
        for i in range(CHUNK // LANES):
            row = p * (CHUNK // LANES) + i
            labrow_f = total[:, i * LANES:(i + 1) * LANES]
            pick_f = chosen[:, i * LANES:(i + 1) * LANES]
            parts[n_all + row, 0:1, :] = labrow_f
            parts[n_all + row, 1:2, :] = pick_f

    for row in range(n_rows):
        total = jnp.zeros((2, LANES), jnp.float32)
        for b in range(group):
            dev = row * group + b
            x, t = (dev // n_t) // 2, jnp.int32(dev % n_t)
            side = (dev // n_t) % 2
            ahead = lax.rem(ring_of(jnp.int32(x), t) - here + chips, chips)
            slot = jnp.where(ahead == 0, 0, jnp.where(ahead < last, 2 * ahead, 2 * (chips - ahead) - 1))
            index = slot * 2 + side
            shift = lax.rem(b - lax.rem(index, group) + group, group) * half
            held = parts[n_all + index // group]
            total = jnp.where(lane // half == b, pltpu.roll(held, shift, 1)[0:2], total)
        mine[row:row + 1, :] = total[0:1]
        mine[n_rows + row:n_rows + row + 1, :] = total[1:2]

    parts[me, 0:2 * n_rows, :] = mine[...]
    others(lambda j: part_copy(me, j).start())
    others(lambda j: part_copy(j, me).wait_recv())

    def add_part(j, carry):
        return carry + parts[j, 0:2 * n_rows, :]
    total = lax.fori_loop(0, n_all, add_part, jnp.zeros((2 * n_rows, LANES), jnp.float32))
    lse = jnp.log(total[0:n_rows])
    picked = total[n_rows:2 * n_rows] * CAP
    spot = lax.broadcasted_iota(jnp.int32, (n_rows, LANES), 0) * LANES + lax.broadcasted_iota(
        jnp.int32, (n_rows, LANES), 1)
    owner, within = spot // half, lax.rem(spot, half)
    batch = owner // n_t * seqs + within // stretch
    position = lax.rem(owner, n_t) * stretch + lax.rem(within, stretch)
    limit = jnp.zeros((n_rows, LANES), jnp.int32)
    for b in range(n_dp * seqs):
        limit = jnp.where(batch == b, lengths_ref[b], limit)
    live = jnp.where((position < limit) & (within < seqs * stretch), 1.0, 0.0)
    token = live * (picked - lse)

    def whole(x):
        return jnp.sum(jnp.sum(x, axis=1, keepdims=True), axis=0, keepdims=True)
    count = whole(live)
    nll = -whole(token) / count
    z_loss = 0.01 * whole(live * lse * lse) / count
    mine_token = jnp.zeros((1, LANES), jnp.float32)
    for row in range(n_rows):
        mine_token = jnp.where(me // group == row, token[row:row + 1], mine_token)
    shift = lax.rem(group - lax.rem(me, group), group) * half
    out_ref[...] = jnp.zeros_like(out_ref)
    out_ref[...] = pltpu.roll(jnp.broadcast_to(mine_token, (8, LANES)), shift, 1)
    out_ref[1:2, :] = jnp.broadcast_to(nll, (1, LANES))
    out_ref[2:3, :] = jnp.broadcast_to(z_loss, (1, LANES))

    def drain(step, carry):
        d = step // 2
        h = lax.rem(step, 2)

        @pl.when(d < reach)
        def _():
            to_next(d, h).wait_send()

        @pl.when((d <= reach) & ((d > 0) | (h == core)))
        def _():
            to_mate(d, h).wait_send()
        return carry
    lax.fori_loop(0, 2 * (last + 1), drain, 0)
    others(lambda j: label_copy(me, j).wait_send())
    others(lambda j: part_copy(me, j).wait_send())


def solution(mesh):
    n_dp, n_t = mesh.shape["dp"], mesh.shape["tensor"]

    def per_device(hidden, gain, labels, lengths, embed):
        seqs, stretch, width = hidden.shape
        n_all = n_dp * n_t
        rows_local = seqs * stretch
        half = 16 * pl.cdiv(rows_local, 16)
        vocab_dev = embed.shape[0]
        vt = tile_rows(vocab_dev)
        n_tiles = vocab_dev // vt
        total = n_all * half
        passes = total // CHUNK
        n_slots = min(n_tiles, (56 * 1024 * 1024 - total * width * 2) // (vt * width * 2))
        chips = n_all // 2
        last = chips // 2
        early = min(last, pl.cdiv(CHUNK // (2 * half), 2))
        if passes != 2 or 2 * (last - early) > n_tiles // 2:
            early = last
        n_rows = total // LANES
        flat = jnp.pad(hidden.reshape(rows_local, width), ((0, half - rows_local), (0, 0)))
        own = jnp.pad(labels.reshape(1, rows_local), ((0, 0), (0, half - rows_local)), constant_values=-1)
        own = jnp.tile(own, (1, LANES // half))
        cfg = (n_dp, n_t, half, seqs, stretch, vt, n_tiles, n_slots, last, early)
        vmem = pl.BlockSpec(memory_space=pltpu.VMEM)
        dma = pltpu.SemaphoreType.DMA
        part_rows = max(8, 2 * n_rows)
        out = pl.pallas_call(
            functools.partial(kernel, cfg),
            out_shape=jax.ShapeDtypeStruct((8, LANES), jnp.float32),
            in_specs=[vmem, vmem, vmem, pl.BlockSpec(memory_space=pltpu.SMEM), pl.BlockSpec(memory_space=pl.ANY)],
            out_specs=vmem,
            scratch_shapes=[
                pltpu.VMEM((total, width), jnp.bfloat16),
                pltpu.VMEM((n_slots, vt, width), jnp.bfloat16),
                pltpu.VMEM((vt, CHUNK), jnp.float32),
                pltpu.VMEM((vt, CHUNK), jnp.float32),
                pltpu.VMEM((passes + 1, 8, CHUNK), jnp.float32),
                pltpu.VMEM((passes + 1, 8, CHUNK), jnp.float32),
                pltpu.VMEM((passes, 1, CHUNK), jnp.int32),
                pltpu.VMEM((n_rows, 1, LANES), jnp.int32),
                pltpu.VMEM((n_all, 1, LANES), jnp.int32),
                pltpu.VMEM((2 * n_rows, LANES), jnp.float32),
                pltpu.VMEM((n_all + n_rows, part_rows, LANES), jnp.float32),
                dma((n_slots,)),
                dma((last + 1, 2)), dma((last + 1, 2)), dma((last + 1, 2)), dma((last + 1, 2)),
                dma((n_all,)), dma((n_all,)), dma((n_all,)), dma((n_all,)),
            ],
            compiler_params=pltpu.CompilerParams(
                collective_id=0, has_side_effects=True, vmem_limit_bytes=67043328),
        )(flat, gain.reshape(1, width), own, lengths, embed)
        return out[0, :rows_local].reshape(seqs, stretch), out[1, 0], out[2, 0]

    return jax.shard_map(
        per_device,
        mesh=mesh,
        in_specs=(P("dp", "tensor", None), P(), P("dp", "tensor"), P(), P(("dp", "tensor"), None)),
        out_specs=(P("dp", "tensor"), P(), P()),
        check_vma=False,
    )
```
